32 devices in a mesh: ep: 8 (over y, x, core), tp: 4 (over z).
Axes of the slice: x: 2, y: 2, z: 4, core: 2. Of those that a mesh axis runs over, the one named last changes fastest.
Arguments:
- tokens: bfloat16 [256, 4096], P('ep', 'tp'), may hold values from -6 to 6
- norm_gains: float32 [2, 4096], replicated, may hold values from 0.1 to 1.9
- router: bfloat16 [2, 4096, 16], replicated, as said below
- w_gate: bfloat16 [2, 16, 4096, 768], P(None, 'ep', None, 'tp'), may hold values from -0.09375 to 0.09375
- w_up: bfloat16 [2, 16, 4096, 768], P(None, 'ep', None, 'tp'), may hold values from -0.09375 to 0.09375
- w_down: bfloat16 [2, 16, 768, 4096], P(None, 'ep', 'tp'), may hold values from -0.21875 to 0.21875
- expert_ids: int32 [2, 256, 8], P(None, 'ep'), may hold values from 0 to 15, all different within a row; in each aligned block of 32 rows (0 to 31, 32 to 63, ...) at most 32 rows name the same one
Outputs:
- hidden_out: bfloat16 [256, 4096], P('ep', 'tp')
The draws below stay inside these ranges and needn't reach their ends.
Inputs may be any that keep to these rules, and one draw needn't show every extreme that they name: `expert_ids`: each entry names an expert of 0 to 15; the 8 entries of a token differ; among the 32 tokens of one ep index in one layer no expert is named more than 32 times, and in some such blocks one is named exactly 32 times. `router`: entries of order 2 / sqrt(4096); all columns of a layer may share a common added vector with entries of order 50 / sqrt(4096).
All inputs are finite; a program needn't handle non-finite values.
Results may differ from the reference program's by a relative error of at most 0.02.
Values may be sent and summed in bfloat16 or wider, within the bound.
A program may use at most 64 MiB of HBM per device.

```python
import math
import jax
import jax.numpy as jnp
import numpy as np
from jax import lax

D = 4096
FF = 768
TOP = 8
LAYERS = 2
TOK_DEV = 32
TOKENS = 256
EXPERTS = 16
CAP = 32
N_EP = 8


def draw_router(key, part):
    base = jax.random.normal(jax.random.fold_in(key, 11), (LAYERS, D, EXPERTS), jnp.float32) * (2.0 / math.sqrt(D))
    return base.astype(jnp.bfloat16)


def levels(own_key, shape, pieces, low, high):
    loudness = 1.0
    for axis_at, blocks in pieces:
        steps = jax.random.uniform(jax.random.fold_in(jax.random.fold_in(own_key, 6), axis_at), (blocks,), jnp.float32, low / len(pieces), high / len(pieces))
        loudness = loudness * jnp.repeat(jnp.exp(steps), shape[axis_at] // blocks).reshape((-1,) + (1,) * (len(shape) - 1 - axis_at))
    return loudness


def deal_out(key, own, number, rows, amount, top, limit, slope):
    ranking = jax.random.permutation(key, amount)
    heavy_load, usual = shares(amount, rows * top, limit, slope, True), shares(amount, rows * top, limit, slope, False)
    places = jnp.arange(amount)

    def named(sizes, rotation):
        used = int((sizes > 0).sum())
        fixed = max(1, used // 4)
        moved = fixed + (places - fixed + rotation * (used - fixed)) % max(1, amount - fixed)
        return jnp.zeros((amount,), jnp.int32).at[ranking[jnp.where(places < fixed, places, moved)]].set(jnp.asarray(sizes, jnp.int32))

    sizes = jnp.where(number % 4 == 0, named(heavy_load, number // 4), named(usual, number - number // 4 - 1))
    mixed = jax.random.permutation(jax.random.fold_in(own, 3), amount)
    giver, sink = mixed[0:amount // 2 * 2:2], mixed[1:amount // 2 * 2:2]
    room = jnp.minimum(sizes[giver] - 1, limit - sizes[sink]) // 2
    room = jnp.where((giver == ranking[0]) | (sink == ranking[0]) | (sizes[sink] == 0), 0, jnp.maximum(room, 0))
    moved = jax.random.randint(jax.random.fold_in(own, 4), (amount // 2,), 0, 1 << 20) % (room + 1)
    sizes = sizes.at[giver].add(-moved).at[sink].add(moved)
    labels = jnp.searchsorted(jnp.cumsum(sizes), jnp.arange(rows * top), side="right").astype(jnp.int32)
    grid = labels.reshape(top, rows).T
    grid = grid[jax.random.permutation(jax.random.fold_in(own, 1), rows)]
    rotation = jax.random.randint(jax.random.fold_in(own, 2), (rows, 1), 0, top)
    return jnp.take_along_axis(grid, (jnp.arange(top)[None, :] + rotation) % top, axis=1)


def shares(amount, total, bound, skew, full):
    loads = [(1 << 20) // math.isqrt(rank ** skew) + 1 for rank in range(1, amount + 1)]
    largest = bound if full else min(bound, max(-(-total // amount), total * loads[0] // sum(loads)))
    least = 1 if total - largest >= amount - 1 else 0
    counts, rest = [largest] + [least] * (amount - 1), total - largest - least * (amount - 1)
    while rest > 0:
        candidates = [i for i in range(1, amount) if counts[i] < largest] or [i for i in range(1, amount) if counts[i] < bound]
        pool, budget = sum([loads[i] for i in candidates]), rest
        for i in candidates:
            more = min(bound - counts[i], max(1, budget * loads[i] // pool), rest)
            counts[i] = counts[i] + more
            rest = rest - more
    return np.array(counts)


def gaussian(own_key, shape, spread, limit, cuts=(), kind=jnp.bfloat16):
    drawn = jax.random.normal(own_key, shape, jnp.float32) * spread
    if len(cuts) > 0:
        drawn = levels(own_key, shape, cuts, -0.22, 0.18) * drawn
    return jnp.clip(drawn, min=-limit, max=limit).astype(kind)


def setup_inputs(seed: int = 0) -> dict:
    keys = jax.random.split(jax.random.key(seed), 8)
    tokens = gaussian(keys[0], (TOKENS, D), 1.0, 6.0, ((0, 8), (1, 4)))
    norm_gains = jnp.clip(1.0 + 0.18 * jax.random.normal(keys[1], (LAYERS, D), jnp.float32), 0.1, 1.9)
    router = draw_router(jax.random.fold_in(keys[7], 71), 0)
    w_gate = gaussian(keys[3], (LAYERS, EXPERTS, D, FF), D ** -0.5, 0.09375, ((1, 8), (3, 4)))
    w_up = gaussian(keys[4], (LAYERS, EXPERTS, D, FF), D ** -0.5, 0.09375, ((1, 8), (3, 4)))
    w_down = gaussian(keys[5], (LAYERS, EXPERTS, FF, D), FF ** -0.5, 0.21875, ((1, 8), (2, 4)))
    expert_ids_keys = jax.random.split(jax.random.fold_in(keys[6], 1), LAYERS * TOKENS // TOK_DEV)
    expert_ids_turns = jax.random.permutation(jax.random.fold_in(keys[6], 3), LAYERS * TOKENS // TOK_DEV)
    expert_ids = jax.vmap(lambda own, number: deal_out(jax.random.fold_in(keys[6], 2), own, number, TOK_DEV, EXPERTS, TOP, CAP, 2))(expert_ids_keys, expert_ids_turns).reshape((LAYERS, TOKENS, TOP))
    return dict(tokens=tokens, norm_gains=norm_gains, router=router, w_gate=w_gate, w_up=w_up, w_down=w_down, expert_ids=expert_ids)


norm_eps = 1e-06

def moe_layer(hidden_in, gain, weight, gate_w, up_w, down_w, ids):
    wide_rows = hidden_in.astype(jnp.float32)
    square_sum = lax.optimization_barrier(jnp.sum(wide_rows * wide_rows, axis=1))
    scaled = (wide_rows * gain[None, :]).astype(jnp.bfloat16)
    raw_logits = jnp.dot(scaled, weight, preferred_element_type=jnp.float32)
    inverse = lax.rsqrt(square_sum / D + norm_eps)
    normed = (scaled.astype(jnp.float32) * inverse[:, None]).astype(jnp.bfloat16)
    logits = raw_logits * inverse[:, None]
    picked = jnp.take_along_axis(logits, ids, axis=1)
    gate_probs = jax.nn.softmax(picked, axis=-1)
    flat_ids = ids.reshape(N_EP, TOK_DEV * TOP)
    onehot = (flat_ids[:, :, None] == jnp.arange(EXPERTS, dtype=jnp.int32)[None, None, :]).astype(jnp.int32)
    earlier = jnp.cumsum(onehot, axis=1) - onehot
    slot_index = lax.optimization_barrier(jnp.sum(earlier * onehot, axis=2)).reshape(TOKENS, TOP).astype(jnp.int32)
    block_index = jnp.broadcast_to((jnp.arange(TOKENS, dtype=jnp.int32) // TOK_DEV)[:, None], (TOKENS, TOP))
    buffer = jnp.zeros((EXPERTS, N_EP, CAP, D), jnp.bfloat16)
    buffer = buffer.at[ids, block_index, slot_index].set(jnp.broadcast_to(normed[:, None, :], (TOKENS, TOP, D)))
    rows_all = buffer.reshape(EXPERTS, N_EP * CAP, D)

    def expert_block(operands):
        rows_e, gate_e, up_e, down_e = operands
        gate_proj = jnp.dot(rows_e, gate_e, preferred_element_type=jnp.float32)
        up_proj = jnp.dot(rows_e, up_e, preferred_element_type=jnp.float32)
        inner = (jax.nn.silu(gate_proj) * up_proj).astype(jnp.bfloat16)
        return jnp.dot(inner, down_e, preferred_element_type=jnp.float32).astype(jnp.bfloat16)
    outputs = lax.map(expert_block, (rows_all, gate_w, up_w, down_w))
    outputs = outputs.reshape(EXPERTS, N_EP, CAP, D)
    gathered = outputs[ids, block_index, slot_index].astype(jnp.float32)
    moe_out = lax.optimization_barrier(jnp.sum(gate_probs[:, :, None] * gathered, axis=1))
    return (wide_rows + moe_out).astype(jnp.bfloat16)

def reference(tokens, norm_gains, router, w_gate, w_up, w_down, expert_ids):
    current = tokens
    for layer_idx in range(LAYERS):
        current = moe_layer(current, norm_gains[layer_idx], router[layer_idx], w_gate[layer_idx], w_up[layer_idx], w_down[layer_idx], expert_ids[layer_idx])
    return current
```

```python
import functools

import jax
import jax.numpy as jnp
from jax import lax
from jax.experimental import pallas as pl
from jax.experimental.pallas import tpu as pltpu
from jax.sharding import PartitionSpec as P

MESH = pl.DeviceIdType.MESH
BF16, F32 = jnp.bfloat16, jnp.float32
CORES = 2
LANES = 128

norm_eps = 1e-06


def kernel(
    n_ep, n_tp, layers,
    tokens, gains, router, w_gate, w_up, w_down, ids,
    out,
    x, mask, w_in, wd, acc, sacc, inner, own, pair_out, pair_in, plane_out, plane_in,
    line_out, line_in,
    w_sem, mask_send, mask_recv, x_send, x_recv, pair_send, pair_recv, plane_send, plane_recv,
    line_send, line_recv,
):
    rows, width = tokens.shape
    chips = n_ep // CORES
    half = chips * rows
    local_exp, hidden_units = w_gate.shape[1:3]
    experts, top = router.shape[1], ids.shape[1]
    held = local_exp * hidden_units
    me, z = lax.axis_index("ep"), lax.axis_index("tp")
    q, c = me // CORES, lax.rem(me, CORES)
    sibling = (q * CORES + 1 - c, z)

    def chip(k):
        return lax.rem(q + k, chips)

    def plane_dev(k):
        return (chip(k) * CORES + c, z)

    def line_dev(k):
        return (me, lax.rem(z + k, n_tp))

    def at_rows(index, base=0):
        return pl.ds(pl.multiple_of(base + index * rows, rows), rows)

    def columns(dz):
        return pl.ds(pl.multiple_of(lax.rem(z + dz, n_tp) * width, width), width)

    def weight_copies(l):
        pairs = [(router.at[l], w_in.at[l, pl.ds(2 * held, experts), :])]
        for i, source in enumerate((w_gate, w_up)):
            for e in range(local_exp):
                place = pl.ds(i * held + e * hidden_units, hidden_units)
                pairs.append((source.at[l, e], w_in.at[l, place, :]))
        pairs.append((w_down.at[l], wd.at[l]))
        return [
            pltpu.make_async_copy(src, dst, w_sem.at[l, i]) for i, (src, dst) in enumerate(pairs)
        ]

    for l in range(layers):
        for copy in weight_copies(l):
            copy.start()

    barrier = pltpu.get_barrier_semaphore()
    for k in range(1, n_ep):
        pl.semaphore_signal(
            barrier, inc=1, device_id=(lax.rem(me + k, n_ep), z), device_id_type=MESH
        )
    for k in range(1, n_tp):
        pl.semaphore_signal(barrier, inc=1, device_id=line_dev(k), device_id_type=MESH)

    x[0, 0, at_rows(q), :] = tokens[...]
    lane = lax.broadcasted_iota(jnp.int32, (rows, mask.shape[2]), 1)
    for l in range(layers):
        chosen = ids[l].T
        hit = chosen[:, 0:1] == lane
        for k in range(1, top):
            hit = hit | (chosen[:, k : k + 1] == lane)
        mask[l, at_rows(q), :] = jnp.where(hit, 1.0, 0.0).astype(BF16)

    pl.semaphore_wait(barrier, n_ep - 1 + n_tp - 1)

    def remote(src, dst, send, recv, device):
        return pltpu.make_async_remote_copy(
            src_ref=src, dst_ref=dst, send_sem=send, recv_sem=recv,
            device_id=device, device_id_type=MESH,
        )

    mask_copies = []
    for k in range(1, n_ep):
        mask_copies.append(
            remote(
                mask.at[:, at_rows(q), :],
                mask.at[:, at_rows(q, (k % CORES) * half), :],
                mask_send.at[k], mask_recv.at[k],
                (lax.rem(me + k, n_ep), z),
            )
        )

    def layer(l, carry):
        sends = []

        def go(copy):
            copy.start()
            sends.append(copy)

        def to_line(k):
            there = (-k) % n_tp
            mine = x.at[l, 0, at_rows(q), :]
            return remote(
                mine, x.at[l, there, at_rows(q), :],
                x_send.at[l, 0, k, 0], x_recv.at[l, 0, there, q], line_dev(k),
            )

        def to_plane(dz, k):
            ref = x.at[l, dz, at_rows(q), :]
            return remote(
                ref, ref, x_send.at[l, 1, dz, k], x_recv.at[l, 0, dz, q], plane_dev(k)
            )

        def to_sibling(dz, k):
            return remote(
                x.at[l, dz, at_rows(chip(k)), :],
                x.at[l, dz, at_rows(chip(k), half), :],
                x_send.at[l, 2, dz, k], x_recv.at[l, 1, dz, chip(k)], sibling,
            )

        def arrive(parity, dz, k):
            ref = x.at[l, dz, at_rows(chip(k), parity * half), :]
            pltpu.make_async_remote_copy(
                src_ref=ref, dst_ref=ref, send_sem=x_send.at[l, 0, 0, 0],
                recv_sem=x_recv.at[l, parity, dz, chip(k)],
                device_id=sibling, device_id_type=MESH,
            ).wait_recv()

        order = sorted(range(n_tp), key=lambda k: min(k, n_tp - k))
        for k in range(1, n_tp):
            go(to_line(k))
        for k in range(1, chips):
            go(to_plane(0, k))
        go(to_sibling(0, 0))

        @pl.when(l == 0)
        def _():
            for copy in mask_copies:
                copy.start()

        for dz in order[1:]:
            arrive(0, dz, 0)
            for k in range(1, chips):
                go(to_plane(dz, k))
            go(to_sibling(dz, 0))

        for copy in weight_copies(l)[:-1]:
            copy.wait()
        for i, dz in enumerate(order):
            for k in range(1, chips):
                arrive(0, dz, k)
                go(to_sibling(dz, k))
            for k in range(chips):
                arrive(1, dz, k)
            block = x[l, dz].astype(F32)
            square = jnp.sum(block * block, axis=1, keepdims=True)
            scaled = (block * gains[pl.ds(l, 1), columns(dz)]).astype(BF16)
            sums = lax.dot_general(
                scaled, w_in[l, :, columns(dz)], (((1,), (1,)), ((), ())),
                preferred_element_type=F32,
            )
            if i == 0:
                sacc[...] = square
                acc[...] = sums
            else:
                sacc[...] += square
                acc[...] += sums

        @pl.when(l == 0)
        def _():
            for copy in mask_copies:
                copy.wait_recv()

        inverse = lax.rsqrt(sacc[...] / (width * n_tp) + norm_eps)
        logits = acc[:, 2 * held :] * inverse
        hit = mask[l][:, :experts].astype(F32) > 0.5
        logits = jnp.where(hit, logits, -jnp.inf)
        grown = jnp.exp(logits - jnp.max(logits, axis=1, keepdims=True))
        gates = grown / jnp.sum(grown, axis=1, keepdims=True)
        expert = lax.broadcasted_iota(jnp.int32, gates.shape, 1)
        unit = lax.broadcasted_iota(jnp.int32, (1, held), 1)
        weight = None
        for e in range(local_exp):
            gate = jnp.sum(
                jnp.where(expert == me * local_exp + e, gates, 0.0), axis=1, keepdims=True
            )
            weight = gate if e == 0 else jnp.where(unit < e * hidden_units, weight, gate)
        v = acc[:, :held] * inverse
        u = acc[:, held : 2 * held] * inverse
        inner[...] = (v / (1.0 + jnp.exp(-v)) * u * weight).astype(BF16)

        weight_copies(l)[-1].wait()

        def project(dz):
            total = jnp.dot(inner[...], wd[l, :, columns(dz)], preferred_element_type=F32)
            pair_out[dz] = total[half:].astype(BF16)
            own[dz] = total[:half]
            go(remote(
                pair_out.at[dz], pair_in.at[dz],
                pair_send.at[l, dz], pair_recv.at[l, dz], sibling,
            ))

        def landed(ref, send, recv):
            pltpu.make_async_remote_copy(
                src_ref=ref, dst_ref=ref, send_sem=send, recv_sem=recv,
                device_id=sibling, device_id_type=MESH,
            ).wait_recv()

        def spread(dz):
            landed(pair_in.at[dz], pair_send.at[l, dz], pair_recv.at[l, dz])
            total = own[dz] + pair_in[dz].astype(F32)
            own[dz] = total
            plane_out[dz] = total.astype(BF16)
            for k in range(1, chips):
                there = (-k) % chips
                go(remote(
                    plane_out.at[dz, at_rows(chip(k)), :], plane_in.at[l, dz, there],
                    plane_send.at[l, dz, k], plane_recv.at[l, dz, there], plane_dev(k),
                ))

        def gather(dz):
            total = own[dz, at_rows(q), :]
            for k in range(1, chips):
                landed(
                    plane_in.at[l, dz, k], plane_send.at[l, dz, k], plane_recv.at[l, dz, k]
                )
                total = total + plane_in[l, dz, k].astype(F32)
            return total

        back = order[::-1]
        for i, dz in enumerate(back):
            project(dz)
            if i > 0:
                spread(back[i - 1])
        spread(back[-1])
        moe = None
        for dz in back:
            moe = gather(dz)
            if dz != 0:
                there = (-dz) % n_tp
                line_out[l, dz] = moe.astype(BF16)
                go(remote(
                    line_out.at[l, dz], line_in.at[l, there],
                    line_send.at[l, dz], line_recv.at[l, there], line_dev(dz),
                ))
        for k in order[1:]:
            landed(line_in.at[l, k], line_send.at[l, k], line_recv.at[l, k])
            moe = moe + line_in[l, k].astype(F32)
        hidden = (x[l, 0, at_rows(q), :].astype(F32) + moe).astype(BF16)
        for copy in sends:
            copy.wait_send()
        out[...] = hidden

        @pl.when(l < layers - 1)
        def _():
            x[lax.rem(l + 1, layers), 0, at_rows(q), :] = hidden

        return carry

    lax.fori_loop(0, layers, layer, 0)
    for copy in mask_copies:
        copy.wait_send()


def body(tokens, norm_gains, router, w_gate, w_up, w_down, expert_ids):
    n_ep, n_tp = lax.axis_size("ep"), lax.axis_size("tp")
    layers, local_exp, full, hidden = w_gate.shape
    experts = router.shape[2]
    rows, width = tokens.shape
    held = local_exp * hidden
    chips = n_ep // CORES
    every, half = n_ep * rows, chips * rows
    vmem = pl.BlockSpec(memory_space=pltpu.VMEM)
    hbm = pl.BlockSpec(memory_space=pl.ANY)
    dma = pltpu.SemaphoreType.DMA
    lanes = -(-experts // LANES) * LANES
    return pl.pallas_call(
        functools.partial(kernel, n_ep, n_tp, layers),
        out_shape=jax.ShapeDtypeStruct((rows, width), BF16),
        in_specs=[vmem, vmem, vmem, hbm, hbm, hbm, vmem],
        out_specs=vmem,
        scratch_shapes=[
            pltpu.VMEM((layers, n_tp, every, width), BF16),
            pltpu.VMEM((layers, every, lanes), BF16),
            pltpu.VMEM((layers, 2 * held + experts, full), BF16),
            pltpu.VMEM((layers, held, full), BF16),
            pltpu.VMEM((every, 2 * held + experts), F32),
            pltpu.VMEM((every, 1), F32),
            pltpu.VMEM((every, held), BF16),
            pltpu.VMEM((n_tp, half, width), F32),
            pltpu.VMEM((n_tp, half, width), BF16),
            pltpu.VMEM((n_tp, half, width), BF16),
            pltpu.VMEM((n_tp, half, width), BF16),
            pltpu.VMEM((layers, n_tp, chips, rows, width), BF16),
            pltpu.VMEM((layers, n_tp, rows, width), BF16),
            pltpu.VMEM((layers, n_tp, rows, width), BF16),
            dma((layers, 2 + 2 * local_exp)),
            dma((n_ep,)),
            dma((n_ep,)),
            dma((layers, 3, n_tp, chips)),
            dma((layers, 2, n_tp, chips)),
            dma((layers, n_tp)),
            dma((layers, n_tp)),
            dma((layers, n_tp, chips)),
            dma((layers, n_tp, chips)),
            dma((layers, n_tp)),
            dma((layers, n_tp)),
        ],
        compiler_params=pltpu.CompilerParams(
            collective_id=0, has_side_effects=True, vmem_limit_bytes=67043328
        ),
    )(
        tokens, norm_gains, router.swapaxes(1, 2), w_gate.swapaxes(2, 3), w_up.swapaxes(2, 3),
        w_down.reshape(layers, held, full), expert_ids.swapaxes(1, 2),
    )


def solution(mesh):
    in_specs = (
        P("ep", "tp"),
        P(),
        P(),
        P(None, "ep", None, "tp"),
        P(None, "ep", None, "tp"),
        P(None, "ep", "tp", None),
        P(None, "ep", None),
    )
    return jax.shard_map(
        body, mesh=mesh, in_specs=in_specs, out_specs=P("ep", "tp"), check_vma=False
    )
```

```python
import functools

import jax
import jax.numpy as jnp
from jax import lax
from jax.experimental import pallas as pl
from jax.experimental.pallas import tpu as pltpu
from jax.sharding import PartitionSpec as P

MESH = pl.DeviceIdType.MESH
BF16, F32 = jnp.bfloat16, jnp.float32
CORES = 2
LANES = 128

norm_eps = 1e-06


def flip(index, k):
    bit = 1
    while bit <= k:
        if k & bit:
            index = index + bit * (1 - 2 * lax.rem(index // bit, 2))
        bit *= 2
    return index


def kernel(
    n_ep, n_tp, layers,
    tokens, gains, router, w_gate, w_up, w_down, ids,
    out,
    x, mask, w_in, wd, acc, sacc, inner, own, pair_out, pair_in, plane_out, plane_in,
    line_out, line_in,
    w_sem, mask_send, mask_recv, x_send, x_recv, pair_send, pair_recv, plane_send, plane_recv,
    line_send, line_recv,
):
    rows, width = tokens.shape
    chips = n_ep // CORES
    half = chips * rows
    local_exp, hidden_units = w_gate.shape[1:3]
    experts, top = router.shape[1], ids.shape[1]
    held = local_exp * hidden_units
    me, z = lax.axis_index("ep"), lax.axis_index("tp")
    q, c = me // CORES, lax.rem(me, CORES)
    sibling = (q * CORES + 1 - c, z)

    relay = chips == 4

    def chip(k):
        if relay and 0 < k < 3:
            one, two = flip(q, k), flip(q, 3 - k)
            return one + c * (two - one)
        return flip(q, k)

    def plane_dev(k):
        return (chip(k) * CORES + c, z)

    def line_dev(k):
        return (me, flip(z, k))

    def at_rows(index, base=0):
        return pl.ds(pl.multiple_of(base + index * rows, rows), rows)

    def columns(dz):
        return pl.ds(pl.multiple_of(flip(z, dz) * width, width), width)

    def weight_copies(l):
        pairs = [(router.at[l], w_in.at[l, pl.ds(2 * held, experts), :])]
        for i, source in enumerate((w_gate, w_up)):
            for e in range(local_exp):
                place = pl.ds(i * held + e * hidden_units, hidden_units)
                pairs.append((source.at[l, e], w_in.at[l, place, :]))
        pairs.append((w_down.at[l], wd.at[l]))
        return [
            pltpu.make_async_copy(src, dst, w_sem.at[l, i]) for i, (src, dst) in enumerate(pairs)
        ]

    for l in range(layers):
        for copy in weight_copies(l):
            copy.start()

    barrier = pltpu.get_barrier_semaphore()
    for k in range(1, n_ep):
        pl.semaphore_signal(
            barrier, inc=1, device_id=(lax.rem(me + k, n_ep), z), device_id_type=MESH
        )
    for k in range(1, n_tp):
        pl.semaphore_signal(barrier, inc=1, device_id=line_dev(k), device_id_type=MESH)

    x[0, 0, at_rows(q), :] = tokens[...]
    lane = lax.broadcasted_iota(jnp.int32, (rows, mask.shape[1]), 1)
    hit = None
    for l in range(layers):
        chosen = ids[l].T + l * experts
        for k in range(top):
            named = chosen[:, k : k + 1] == lane
            hit = named if hit is None else hit | named
    mask[at_rows(q), :] = jnp.where(hit, 1.0, 0.0).astype(BF16)

    pl.semaphore_wait(barrier, n_ep - 1 + n_tp - 1)

    def remote(src, dst, send, recv, device):
        return pltpu.make_async_remote_copy(
            src_ref=src, dst_ref=dst, send_sem=send, recv_sem=recv,
            device_id=device, device_id_type=MESH,
        )

    mask_copies = []
    for k in range(1, n_ep):
        mask_copies.append(
            remote(
                mask.at[at_rows(q), :],
                mask.at[at_rows(q, (k % CORES) * half), :],
                mask_send.at[k], mask_recv.at[k],
                (lax.rem(me + k, n_ep), z),
            )
        )

    def layer(l, carry):
        sends = []

        def go(copy):
            copy.start()
            sends.append(copy)

        def to_line(k):
            mine = x.at[l, 0, at_rows(q), :]
            return remote(
                mine, x.at[l, k, at_rows(q), :],
                x_send.at[l, 0, k, 0], x_recv.at[l, 0, k, q], line_dev(k),
            )

        def to_plane(dz, k):
            ref = x.at[l, dz, at_rows(q), :]
            return remote(
                ref, ref, x_send.at[l, 1, dz, k], x_recv.at[l, 0, dz, q], plane_dev(k)
            )

        def onward(dz):
            ref = x.at[l, dz, at_rows(chip(1)), :]
            return remote(
                ref, ref, x_send.at[l, 1, dz, 3], x_recv.at[l, 0, dz, chip(1)], plane_dev(2)
            )

        def to_sibling(dz, k):
            return remote(
                x.at[l, dz, at_rows(chip(k)), :],
                x.at[l, dz, at_rows(chip(k), half), :],
                x_send.at[l, 2, dz, k], x_recv.at[l, 1, dz, chip(k)], sibling,
            )

        def arrive(parity, dz, k):
            ref = x.at[l, dz, at_rows(chip(k), parity * half), :]
            pltpu.make_async_remote_copy(
                src_ref=ref, dst_ref=ref, send_sem=x_send.at[l, 0, 0, 0],
                recv_sem=x_recv.at[l, parity, dz, chip(k)],
                device_id=sibling, device_id_type=MESH,
            ).wait_recv()

        near = range(1, 3 if relay else chips)
        for k in range(1, n_tp):
            go(to_line(k))
        for k in near:
            go(to_plane(0, k))
        go(to_sibling(0, 0))

        @pl.when(l == 0)
        def _():
            for copy in mask_copies:
                copy.start()

        def pass_on(dz):
            if dz + 1 < n_tp:
                arrive(0, dz + 1, 0)
                for k in near:
                    go(to_plane(dz + 1, k))
                go(to_sibling(dz + 1, 0))
            for k in near:
                arrive(0, dz, k)
                if relay and k == 1:
                    go(onward(dz))
                go(to_sibling(dz, k))

        def complete(dz):
            if relay:
                arrive(0, dz, 3)
                go(to_sibling(dz, 3))
            for k in range(chips):
                arrive(1, dz, k)
            if dz == 0:
                for copy in weight_copies(l)[:-1]:
                    copy.wait()
            block = x[l, dz].astype(F32)
            square = jnp.sum(block * block, axis=1, keepdims=True)
            scaled = (block * gains[pl.ds(l, 1), columns(dz)]).astype(BF16)
            sums = lax.dot_general(
                scaled, w_in[l, :, columns(dz)], (((1,), (1,)), ((), ())),
                preferred_element_type=F32,
            )
            if dz == 0:
                sacc[...] = square
                acc[...] = sums
            else:
                sacc[...] += square
                acc[...] += sums

        for dz in range(n_tp):
            pass_on(dz)
            if dz > 0:
                complete(dz - 1)
        complete(n_tp - 1)

        @pl.when(l == 0)
        def _():
            for copy in mask_copies:
                copy.wait_recv()

        inverse = lax.rsqrt(sacc[...] / (width * n_tp) + norm_eps)
        logits = acc[:, 2 * held :] * inverse
        hit = mask[:, :experts].astype(F32)
        for n in range(1, layers):
            hit = jnp.where(l == n, mask[:, n * experts : (n + 1) * experts].astype(F32), hit)
        logits = jnp.where(hit > 0.5, logits, -jnp.inf)
        grown = jnp.exp(logits - jnp.max(logits, axis=1, keepdims=True))
        gates = grown / jnp.sum(grown, axis=1, keepdims=True)
        expert = lax.broadcasted_iota(jnp.int32, gates.shape, 1)
        unit = lax.broadcasted_iota(jnp.int32, (1, held), 1)
        weight = None
        for e in range(local_exp):
            gate = jnp.sum(
                jnp.where(expert == me * local_exp + e, gates, 0.0), axis=1, keepdims=True
            )
            weight = gate if e == 0 else jnp.where(unit < e * hidden_units, weight, gate)
        v = acc[:, :held] * inverse
        u = acc[:, held : 2 * held] * inverse
        inner[...] = (v / (1.0 + jnp.exp(-v)) * u * weight).astype(BF16)

        weight_copies(l)[-1].wait()

        def project(dz):
            total = jnp.dot(inner[...], wd[l, :, columns(dz)], preferred_element_type=F32)
            pair_out[dz] = total[half:].astype(BF16)
            own[dz] = total[:half]
            go(remote(
                pair_out.at[dz], pair_in.at[dz],
                pair_send.at[l, dz], pair_recv.at[l, dz], sibling,
            ))

        def landed(ref, send, recv):
            pltpu.make_async_remote_copy(
                src_ref=ref, dst_ref=ref, send_sem=send, recv_sem=recv,
                device_id=sibling, device_id_type=MESH,
            ).wait_recv()

        def spread(dz):
            landed(pair_in.at[dz], pair_send.at[l, dz], pair_recv.at[l, dz])
            total = own[dz] + pair_in[dz].astype(F32)
            own[dz] = total
            plane_out[dz] = total.astype(BF16)
            if relay:
                go(plane_copy(dz, chip(3), 3, 2))
                go(plane_copy(dz, chip(2), 2, 2))
            else:
                for k in near:
                    go(plane_copy(dz, chip(k), k, k))

        def plane_copy(dz, place, slot, k):
            return remote(
                plane_out.at[dz, at_rows(place), :], plane_in.at[l, dz, slot],
                plane_send.at[l, dz, slot], plane_recv.at[l, dz, slot], plane_dev(k),
            )

        def plane_landed(dz, slot):
            landed(
                plane_in.at[l, dz, slot], plane_send.at[l, dz, slot], plane_recv.at[l, dz, slot]
            )
            return plane_in[l, dz, slot].astype(F32)

        def add_on(dz):
            if relay:
                both = own[dz, at_rows(chip(1)), :] + plane_landed(dz, 3)
                plane_out[dz, at_rows(chip(1)), :] = both.astype(BF16)
                go(plane_copy(dz, chip(1), 1, 1))

        def gather(dz):
            total = own[dz, at_rows(q), :]
            for k in near:
                total = total + plane_landed(dz, k)
            if dz != 0:
                line_out[l, dz] = total.astype(BF16)
                go(remote(
                    line_out.at[l, dz], line_in.at[l, dz],
                    line_send.at[l, dz], line_recv.at[l, dz], line_dev(dz),
                ))
            return total

        back = list(range(n_tp))[::-1]
        for i, dz in enumerate(back):
            project(dz)
            if i > 0:
                spread(back[i - 1])
        spread(back[-1])
        for i, dz in enumerate(back):
            add_on(dz)
            if i > 0:
                gather(back[i - 1])
        moe = gather(back[-1])
        for k in back[:-1]:
            landed(line_in.at[l, k], line_send.at[l, k], line_recv.at[l, k])
            moe = moe + line_in[l, k].astype(F32)
        hidden = (x[l, 0, at_rows(q), :].astype(F32) + moe).astype(BF16)
        for copy in sends:
            copy.wait_send()
        out[...] = hidden

        @pl.when(l < layers - 1)
        def _():
            x[lax.rem(l + 1, layers), 0, at_rows(q), :] = hidden

        return carry

    lax.fori_loop(0, layers, layer, 0)
    for copy in mask_copies:
        copy.wait_send()


def body(tokens, norm_gains, router, w_gate, w_up, w_down, expert_ids):
    n_ep, n_tp = lax.axis_size("ep"), lax.axis_size("tp")
    layers, local_exp, full, hidden = w_gate.shape
    experts = router.shape[2]
    rows, width = tokens.shape
    held = local_exp * hidden
    chips = n_ep // CORES
    every, half = n_ep * rows, chips * rows
    vmem = pl.BlockSpec(memory_space=pltpu.VMEM)
    hbm = pl.BlockSpec(memory_space=pl.ANY)
    dma = pltpu.SemaphoreType.DMA
    lanes = -(-layers * experts // LANES) * LANES
    return pl.pallas_call(
        functools.partial(kernel, n_ep, n_tp, layers),
        out_shape=jax.ShapeDtypeStruct((rows, width), BF16),
        in_specs=[vmem, vmem, vmem, hbm, hbm, hbm, vmem],
        out_specs=vmem,
        scratch_shapes=[
            pltpu.VMEM((layers, n_tp, every, width), BF16),
            pltpu.VMEM((every, lanes), BF16),
            pltpu.VMEM((layers, 2 * held + experts, full), BF16),
            pltpu.VMEM((layers, held, full), BF16),
            pltpu.VMEM((every, 2 * held + experts), F32),
            pltpu.VMEM((every, 1), F32),
            pltpu.VMEM((every, held), BF16),
            pltpu.VMEM((n_tp, half, width), F32),
            pltpu.VMEM((n_tp, half, width), BF16),
            pltpu.VMEM((n_tp, half, width), BF16),
            pltpu.VMEM((n_tp, half, width), BF16),
            pltpu.VMEM((layers, n_tp, chips, rows, width), BF16),
            pltpu.VMEM((layers, n_tp, rows, width), BF16),
            pltpu.VMEM((layers, n_tp, rows, width), BF16),
            dma((layers, 2 + 2 * local_exp)),
            dma((n_ep,)),
            dma((n_ep,)),
            dma((layers, 3, n_tp, chips)),
            dma((layers, 2, n_tp, chips)),
            dma((layers, n_tp)),
            dma((layers, n_tp)),
            dma((layers, n_tp, chips)),
            dma((layers, n_tp, chips)),
            dma((layers, n_tp)),
            dma((layers, n_tp)),
        ],
        compiler_params=pltpu.CompilerParams(
            collective_id=0, has_side_effects=True, vmem_limit_bytes=67043328
        ),
    )(
        tokens, norm_gains, router.swapaxes(1, 2), w_gate.swapaxes(2, 3), w_up.swapaxes(2, 3),
        w_down.reshape(layers, held, full), expert_ids.swapaxes(1, 2),
    )


def solution(mesh):
    in_specs = (
        P("ep", "tp"),
        P(),
        P(),
        P(None, "ep", None, "tp"),
        P(None, "ep", None, "tp"),
        P(None, "ep", "tp", None),
        P(None, "ep", None),
    )
    return jax.shard_map(
        body, mesh=mesh, in_specs=in_specs, out_specs=P("ep", "tp"), check_vma=False
    )
```

```python
import functools

import jax
import jax.numpy as jnp
from jax import lax
from jax.experimental import pallas as pl
from jax.experimental.pallas import tpu as pltpu
from jax.sharding import PartitionSpec as P

MESH = pl.DeviceIdType.MESH
BF16, F32 = jnp.bfloat16, jnp.float32
CORES = 2
LANES = 128
PIECES = 1

norm_eps = 1e-06


def flip(index, k):
    bit = 1
    while bit <= k:
        if k & bit:
            index = index + bit * (1 - 2 * lax.rem(lax.div(index, bit), 2))
        bit *= 2
    return index


def kernel(
    n_ep, n_tp, layers, pieces,
    tokens, gains, router, w_gate, w_up, w_down, ids,
    out,
    x, mask, w_in, wd, acc, sacc, inner, own, pair_out, pair_in, plane_out, plane_in,
    line_out, line_in,
    w_sem, mask_send, mask_recv, x_send, x_recv, pair_send, pair_recv, plane_send, plane_recv,
    line_send, line_recv,
):
    rows, width = tokens.shape[0], tokens.shape[1] // pieces
    chips = n_ep // CORES
    half = chips * rows
    local_exp, hidden_units = w_gate.shape[1:3]
    experts, top = router.shape[1], ids.shape[1]
    held = local_exp * hidden_units
    me, z = lax.axis_index("ep"), lax.axis_index("tp")
    q, c = lax.div(me, CORES), lax.rem(me, CORES)
    sibling = (q * CORES + 1 - c, z)

    relay = chips == 4

    chip_at = [[flip(q, k) for k in range(chips)] for _ in range(2)]
    if relay:
        for odd, at in enumerate(chip_at):
            turn = lax.rem(c + odd, 2) * (at[2] - at[1])
            at[1:3] = [at[1] + turn, at[2] - turn]
    plane_at = [[(i * CORES + c, z) for i in at] for at in chip_at]
    line_at = [(me, flip(z, k)) for k in range(n_tp)]
    first_column = [at * (pieces * width) for _, at in line_at]
    first_row = [[i * rows for i in at] for at in chip_at]

    def row_range(k, base=0, dz=0):
        return pl.ds(pl.multiple_of(base + first_row[dz % 2][k], rows), rows)

    chunks = n_tp * pieces

    def columns(j):
        start = first_column[j // pieces] + j % pieces * width
        return pl.ds(pl.multiple_of(start, width), width)

    def weight_copies(l):
        pairs = [(router.at[l], w_in.at[l, pl.ds(2 * held, experts), :])]
        for i, source in enumerate((w_gate, w_up)):
            for e in range(local_exp):
                place = pl.ds(i * held + e * hidden_units, hidden_units)
                pairs.append((source.at[l, e], w_in.at[l, place, :]))
        pairs.append((w_down.at[l], wd.at[l]))
        return [
            pltpu.make_async_copy(src, dst, w_sem.at[l, i]) for i, (src, dst) in enumerate(pairs)
        ]

    for l in range(layers):
        for copy in weight_copies(l):
            copy.start()

    barrier = pltpu.get_barrier_semaphore()
    for k in range(1, n_ep):
        pl.semaphore_signal(
            barrier, inc=1, device_id=(lax.rem(me + k, n_ep), z), device_id_type=MESH
        )
    for k in range(1, n_tp):
        pl.semaphore_signal(barrier, inc=1, device_id=line_at[k], device_id_type=MESH)

    for p in range(pieces):
        x[0, p, row_range(0), :] = tokens[:, p * width : (p + 1) * width]
    lane = lax.broadcasted_iota(jnp.int32, (rows, mask.shape[1]), 1)
    hit = None
    for l in range(layers):
        chosen = ids[l].T + l * experts
        for k in range(top):
            named = chosen[:, k : k + 1] == lane
            hit = named if hit is None else hit | named
    mask[row_range(0), :] = jnp.where(hit, 1.0, 0.0).astype(BF16)

    pl.semaphore_wait(barrier, n_ep - 1 + n_tp - 1)

    def remote(src, dst, send, recv, device):
        return pltpu.make_async_remote_copy(
            src_ref=src, dst_ref=dst, send_sem=send, recv_sem=recv,
            device_id=device, device_id_type=MESH,
        )

    mask_copies = []
    for k in range(1, n_ep):
        mask_copies.append(
            remote(
                mask.at[row_range(0), :],
                mask.at[row_range(0, (k % CORES) * half), :],
                mask_send.at[k], mask_recv.at[k],
                (lax.rem(me + k, n_ep), z),
            )
        )

    def layer(l, carry):
        sends = []

        def go(copy):
            copy.start()
            sends.append(copy)

        def to_line(j):
            return remote(
                x.at[l, j % pieces, row_range(0), :], x.at[l, j, row_range(0), :],
                x_send.at[l, 0, j, 0], x_recv.at[l, 0, j, q], line_at[j // pieces],
            )

        def to_plane(dz, k):
            ref = x.at[l, dz, row_range(0), :]
            return remote(
                ref, ref, x_send.at[l, 1, dz, k], x_recv.at[l, 0, dz, q], plane_at[dz % 2][k]
            )

        def onward(dz):
            ref = x.at[l, dz, row_range(1, 0, dz), :]
            return remote(
                ref, ref, x_send.at[l, 1, dz, 3], x_recv.at[l, 0, dz, chip_at[dz % 2][1]], plane_at[dz % 2][2]
            )

        def to_sibling(dz):
            return remote(
                x.at[l, dz, pl.ds(0, half), :], x.at[l, dz, pl.ds(half, half), :],
                x_send.at[l, 2, dz, 0], x_recv.at[l, 1, dz, 0], sibling,
            )

        def arrive(parity, dz, k):
            ref = x.at[l, dz, row_range(k, parity * half, dz), :]
            pltpu.make_async_remote_copy(
                src_ref=ref, dst_ref=ref, send_sem=x_send.at[l, 0, 0, 0],
                recv_sem=x_recv.at[l, parity, dz, chip_at[dz % 2][k]],
                device_id=sibling, device_id_type=MESH,
            ).wait_recv()

        near = range(1, 3 if relay else chips)
        for j in range(pieces, chunks):
            go(to_line(j))
        for j in range(pieces):
            for k in near:
                go(to_plane(j, k))

        @pl.when(l == 0)
        def _():
            for copy in mask_copies:
                copy.start()

        def pass_on(dz):
            ahead = dz + pieces
            if ahead < chunks:
                arrive(0, ahead, 0)
                for k in near:
                    go(to_plane(ahead, k))
            for k in near:
                arrive(0, dz, k)
                if relay and k == 1:
                    go(onward(dz))

        def complete(dz):
            if relay:
                arrive(0, dz, 3)
            both = to_sibling(dz)
            go(both)
            both.wait_recv()
            if dz == 0:
                for copy in weight_copies(l)[:-1]:
                    copy.wait()
            block = x[l, dz].astype(F32)
            square = jnp.sum(block * block, axis=1, keepdims=True)
            scaled = (block * gains[pl.ds(l, 1), columns(dz)]).astype(BF16)
            sums = lax.dot_general(
                scaled, w_in[l, :, columns(dz)], (((1,), (1,)), ((), ())),
                preferred_element_type=F32,
            )
            if dz == 0:
                sacc[...] = square
                acc[...] = sums
            else:
                sacc[...] += square
                acc[...] += sums

        for dz in range(chunks):
            pass_on(dz)
            if dz > 0:
                complete(dz - 1)
        complete(chunks - 1)

        @pl.when(l == 0)
        def _():
            for copy in mask_copies:
                copy.wait_recv()

        inverse = lax.rsqrt(sacc[...] / (width * chunks) + norm_eps)
        logits = acc[:, 2 * held :] * inverse
        hit = mask[:, :experts].astype(F32)
        for n in range(1, layers):
            hit = jnp.where(l == n, mask[:, n * experts : (n + 1) * experts].astype(F32), hit)
        logits = jnp.where(hit > 0.5, logits, -jnp.inf)
        grown = jnp.exp(logits - jnp.max(logits, axis=1, keepdims=True))
        gates = grown / jnp.sum(grown, axis=1, keepdims=True)
        expert = lax.broadcasted_iota(jnp.int32, gates.shape, 1)
        unit = lax.broadcasted_iota(jnp.int32, (1, held), 1)
        weight = None
        for e in range(local_exp):
            gate = jnp.sum(
                jnp.where(expert == me * local_exp + e, gates, 0.0), axis=1, keepdims=True
            )
            weight = gate if e == 0 else jnp.where(unit < e * hidden_units, weight, gate)
        v = acc[:, :held] * inverse
        u = acc[:, held : 2 * held] * inverse
        inner[...] = (v / (1.0 + jnp.exp(-v)) * u * weight).astype(BF16)

        weight_copies(l)[-1].wait()

        def project(dz):
            total = jnp.dot(inner[...], wd[l, :, columns(dz)], preferred_element_type=F32)
            pair_out[dz] = total[half:].astype(BF16)
            own[dz] = total[:half]
            go(remote(
                pair_out.at[dz], pair_in.at[dz],
                pair_send.at[l, dz], pair_recv.at[l, dz], sibling,
            ))

        def landed(ref, send, recv):
            pltpu.make_async_remote_copy(
                src_ref=ref, dst_ref=ref, send_sem=send, recv_sem=recv,
                device_id=sibling, device_id_type=MESH,
            ).wait_recv()

        def spread(dz):
            landed(pair_in.at[dz], pair_send.at[l, dz], pair_recv.at[l, dz])
            total = own[dz] + pair_in[dz].astype(F32)
            own[dz] = total
            plane_out[dz] = total.astype(BF16)
            if relay:
                go(plane_copy(dz, 3, 3, 2))
                go(plane_copy(dz, 2, 2, 2))
            else:
                for k in near:
                    go(plane_copy(dz, k, k, k))

        def plane_copy(dz, place, slot, k):
            return remote(
                plane_out.at[dz, row_range(place, 0, dz), :], plane_in.at[l, dz, slot],
                plane_send.at[l, dz, slot], plane_recv.at[l, dz, slot], plane_at[dz % 2][k],
            )

        def plane_landed(dz, slot):
            landed(
                plane_in.at[l, dz, slot], plane_send.at[l, dz, slot], plane_recv.at[l, dz, slot]
            )
            return plane_in[l, dz, slot].astype(F32)

        def add_on(dz):
            if relay:
                both = own[dz, row_range(1, 0, dz), :] + plane_landed(dz, 3)
                plane_out[dz, row_range(1, 0, dz), :] = both.astype(BF16)
                go(plane_copy(dz, 1, 1, 1))

        def gather(dz):
            total = own[dz, row_range(0), :]
            for k in near:
                total = total + plane_landed(dz, k)
            if dz >= pieces:
                line_out[l, dz] = total.astype(BF16)
                go(remote(
                    line_out.at[l, dz], line_in.at[l, dz],
                    line_send.at[l, dz], line_recv.at[l, dz], line_at[dz // pieces],
                ))
            return total

        back = [d * pieces + p for d in reversed(range(n_tp)) for p in range(pieces)]
        for i, dz in enumerate(back):
            project(dz)
            if i > 0:
                spread(back[i - 1])
        spread(back[-1])
        moe = {}
        for i, dz in enumerate(back):
            add_on(dz)
            if i > 0:
                moe[back[i - 1]] = gather(back[i - 1])
        moe[back[-1]] = gather(back[-1])
        hidden = []
        for p in range(pieces):
            total = moe[p]
            for d in reversed(range(1, n_tp)):
                k = d * pieces + p
                landed(line_in.at[l, k], line_send.at[l, k], line_recv.at[l, k])
                total = total + line_in[l, k].astype(F32)
            hidden.append((x[l, p, row_range(0), :].astype(F32) + total).astype(BF16))
        for copy in sends:
            copy.wait_send()
        for p in range(pieces):
            out[:, p * width : (p + 1) * width] = hidden[p]

        @pl.when(l < layers - 1)
        def _():
            for p in range(pieces):
                x[lax.rem(l + 1, layers), p, row_range(0), :] = hidden[p]

        return carry

    lax.fori_loop(0, layers, layer, 0)
    for copy in mask_copies:
        copy.wait_send()


def body(tokens, norm_gains, router, w_gate, w_up, w_down, expert_ids):
    n_ep, n_tp = lax.axis_size("ep"), lax.axis_size("tp")
    layers, local_exp, full, hidden = w_gate.shape
    experts = router.shape[2]
    held = local_exp * hidden
    chips = n_ep // CORES
    pieces = PIECES if chips == 4 else 1
    rows, width = tokens.shape[0], tokens.shape[1] // pieces
    chunks = n_tp * pieces
    every, half = n_ep * rows, chips * rows
    vmem = pl.BlockSpec(memory_space=pltpu.VMEM)
    hbm = pl.BlockSpec(memory_space=pl.ANY)
    dma = pltpu.SemaphoreType.DMA
    lanes = -(-layers * experts // LANES) * LANES
    return pl.pallas_call(
        functools.partial(kernel, n_ep, n_tp, layers, pieces),
        out_shape=jax.ShapeDtypeStruct(tokens.shape, BF16),
        in_specs=[vmem, vmem, vmem, hbm, hbm, hbm, vmem],
        out_specs=vmem,
        scratch_shapes=[
            pltpu.VMEM((layers, chunks, every, width), BF16),
            pltpu.VMEM((every, lanes), BF16),
            pltpu.VMEM((layers, 2 * held + experts, full), BF16),
            pltpu.VMEM((layers, held, full), BF16),
            pltpu.VMEM((every, 2 * held + experts), F32),
            pltpu.VMEM((every, 1), F32),
            pltpu.VMEM((every, held), BF16),
            pltpu.VMEM((chunks, half, width), F32),
            pltpu.VMEM((chunks, half, width), BF16),
            pltpu.VMEM((chunks, half, width), BF16),
            pltpu.VMEM((chunks, half, width), BF16),
            pltpu.VMEM((layers, chunks, chips, rows, width), BF16),
            pltpu.VMEM((layers, chunks, rows, width), BF16),
            pltpu.VMEM((layers, chunks, rows, width), BF16),
            dma((layers, 2 + 2 * local_exp)),
            dma((n_ep,)),
            dma((n_ep,)),
            dma((layers, 3, chunks, chips)),
            dma((layers, 2, chunks, chips)),
            dma((layers, chunks)),
            dma((layers, chunks)),
            dma((layers, chunks, chips)),
            dma((layers, chunks, chips)),
            dma((layers, chunks)),
            dma((layers, chunks)),
        ],
        compiler_params=pltpu.CompilerParams(
            collective_id=0, has_side_effects=True, vmem_limit_bytes=67043328
        ),
    )(
        tokens, norm_gains, router.swapaxes(1, 2), w_gate.swapaxes(2, 3), w_up.swapaxes(2, 3),
        w_down.reshape(layers, held, full), expert_ids.swapaxes(1, 2),
    )


def solution(mesh):
    in_specs = (
        P("ep", "tp"),
        P(),
        P(),
        P(None, "ep", None, "tp"),
        P(None, "ep", None, "tp"),
        P(None, "ep", "tp", None),
        P(None, "ep", None),
    )
    return jax.shard_map(
        body, mesh=mesh, in_specs=in_specs, out_specs=P("ep", "tp"), check_vma=False
    )
```
